32 devices in a mesh: struct: 8 (over z, x), atom: 4 (over y, core).
Axes of the slice: x: 2, y: 2, z: 4, core: 2. Of those that a mesh axis runs over, the one named last changes fastest.
Arguments:
- atoms_in: bfloat16 [32, 1536, 128], P('struct', 'atom'), parts along dimension 0, may hold values from -6 to 6
- cond: bfloat16 [12288, 128], P(('struct', 'atom')), parts along dimension 0, may hold values from -6 to 6
- pair: bfloat16 [384, 32, 16, 128], P(('struct', 'atom')), parts along dimension 0, may hold values from -6 to 6
- atom_mask: int32 [12288], P(('struct', 'atom')), parts along dimension 0, may hold values 0 or 1
- atom_count: int32 [8], P('struct'), parts along dimension 0, may hold values from 1344 to 1536
- atom_to_token: int32 [12288], P(('struct', 'atom')), parts along dimension 0, may hold values from 0 to 191, as said below
- ada_weight: bfloat16 [2, 128, 256], replicated, may hold values from -0.5 to 0.5
- ada_bias: float32 [2, 128], replicated, may hold values from -1.5 to 1.5
- zero_weight: bfloat16 [2, 128, 128], replicated, may hold values from -0.5 to 0.5
- zero_bias: float32 [2, 128], replicated, may hold values from -2 to 2
- qkvg_weight: bfloat16 [128, 512], replicated, may hold values from -0.5 to 0.5
- query_bias: float32 [128], replicated, may hold values from -4 to 4
- pair_weight: float32 [4, 16], replicated, may hold values from -60 to 60
- out_weight: bfloat16 [128, 128], replicated, may hold values from -0.5 to 0.5
- swiglu_weight: bfloat16 [128, 512], replicated, may hold values from -0.5 to 0.5
- down_weight: bfloat16 [256, 128], replicated, may hold values from -0.375 to 0.375
- token_weight: bfloat16 [128, 768], replicated, may hold values from -0.5 to 0.5
Outputs:
- atoms_out: bfloat16 [32, 1536, 128], P('struct', 'atom'), parts along dimension 0
- tokens_out: bfloat16 [32, 192, 768], P('struct', 'atom'), parts along dimension 0
The draws below stay inside these ranges and needn't reach their ends.
There are 8 independent parts, one for each index of `struct`. The reference program is written for one: setup_inputs(seed, part) draws one part's arguments, and reference() takes and returns one part's arrays. A program takes and returns all parts, laid end to end along the dimension named above; an argument that names none is the same for every part. Nothing has to cross between parts.
Inputs may be any that keep to these rules, and one draw needn't show every extreme that they name: `atom_to_token`: never falls, rises by at most 1 from atom to atom, starts at 0 and ends at 191; an atom a of token t satisfies 8 * t - 8 < a < 8 * t + 2 * 8 - 1.
All inputs are finite; a program needn't handle non-finite values. No bound on the sum of `atom_mask` on one device may be relied on, other than what follows from the above.
Results may differ from the reference program's by a relative error of at most 0.01.
Values may be sent and summed in bfloat16 or wider, within the bound.
A program may use at most 64 MiB of HBM per device.

```python
import jax
import jax.numpy as jnp
from jax import lax

C = 128
HEADS = 4
CP = 16
FF = 256
CT = 768
WQ = 32
WK = 128
ATOMS_PER_TOKEN = 8
SAMPLES = 4
ATOM_DEV = 384
ATOMS = 1536
TOKENS = 192
WINDOWS = 48


def draw_atom_to_token(key, part):
    pairs = (TOKENS - 2) // 2
    size = jax.random.randint(jax.random.fold_in(key, 11), (pairs,), 1, ATOMS_PER_TOKEN)
    sign = 2 * jax.random.randint(jax.random.fold_in(key, 13), (pairs,), 0, 2) - 1
    jitter = size * sign
    middle = jnp.stack([ATOMS_PER_TOKEN + jitter, ATOMS_PER_TOKEN - jitter], axis=1).reshape(-1).astype(jnp.int32)
    edge_len = jnp.full((1,), ATOMS_PER_TOKEN, jnp.int32)
    lengths = jnp.concatenate([edge_len, middle, edge_len])
    return jnp.repeat(jnp.arange(TOKENS, dtype=jnp.int32), lengths, total_repeat_length=ATOMS)


def draw_pair_weight(key, part):
    values = jax.random.normal(jax.random.fold_in(key, 23), (HEADS, CP), jnp.float32)
    return jnp.clip(values * 0.5, -2.5, 2.5)


def place_ends(drawn, own_key, low, top_value):
    place = [jax.random.randint(jax.random.fold_in(own_key, axis), (), 0, length) for axis, length in enumerate(drawn.shape)]
    main_axis = drawn.shape.index(max(drawn.shape))
    beside = place[:main_axis] + [(place[main_axis] + 1) % drawn.shape[main_axis]] + place[main_axis + 1:]
    return drawn.at[tuple(place)].set(low).at[tuple(beside)].set(top_value)


def block_scale(rng, dims, split, least, top_value):
    loudness, own = 1.0, jax.random.fold_in(rng, 6)
    for axis_at, shards_of in split:
        heights = jnp.exp(jax.random.uniform(jax.random.fold_in(own, axis_at), (shards_of,), jnp.float32, least / len(split), top_value / len(split)))
        loudness = loudness * jnp.repeat(heights, dims[axis_at] // shards_of).reshape([-1 if axis == axis_at else 1 for axis in range(len(dims))])
    return loudness


def bell_draw(own_key, shape, scale, limit, shards=(), kind=jnp.bfloat16):
    entries = scale * jax.random.normal(own_key, shape, jnp.float32)
    if shards:
        entries = entries * block_scale(own_key, shape, shards, -0.22, 0.18)
    return jnp.clip(entries, -limit, limit).astype(kind)


def setup_inputs(seed: int = 0, part: int = 0) -> dict:
    key_list = jax.random.split(jax.random.key(seed), 18)
    own_keys = jax.random.split(jax.random.fold_in(key_list[17], part), 18)
    return {
        "atoms_in": bell_draw(own_keys[0], (SAMPLES, ATOMS, C), 1.0, 6.0, ((1, 4),)),
        "cond": bell_draw(own_keys[1], (ATOMS, C), 1.0, 6.0, ((0, 4),)),
        "pair": bell_draw(own_keys[2], (WINDOWS, WQ, CP, WK), 1.0, 6.0, ((0, 4),)),
        "atom_mask": place_ends((jax.random.randint(own_keys[3], (ATOMS,), 0, 16) < 15).astype(jnp.int32), jax.random.fold_in(own_keys[3], 1), 0, 1),
        "atom_count": jax.random.randint(own_keys[4], (1,), ATOMS - ATOM_DEV // 2, ATOMS + 1).astype(jnp.int32),
        "atom_to_token": draw_atom_to_token(jax.random.fold_in(jax.random.fold_in(key_list[17], part), 71), part),
        "ada_weight": bell_draw(key_list[6], (2, C, 2 * C), C ** -0.5, 0.5),
        "ada_bias": jnp.clip(jax.random.uniform(key_list[7], (2, C), jnp.float32, -1.5, 1.5), -1.5, 1.5),
        "zero_weight": bell_draw(key_list[8], (2, C, C), C ** -0.5, 0.5),
        "zero_bias": jnp.clip(jax.random.uniform(key_list[9], (2, C), jnp.float32, -2.0, 2.0), -2.0, 2.0),
        "qkvg_weight": bell_draw(key_list[10], (C, 4 * C), C ** -0.5, 0.5),
        "query_bias": bell_draw(key_list[11], (C,), 0.7, 4.0, (), jnp.float32),
        "pair_weight": draw_pair_weight(jax.random.fold_in(key_list[17], 71), part),
        "out_weight": bell_draw(key_list[13], (C, C), C ** -0.5, 0.5),
        "swiglu_weight": bell_draw(key_list[14], (C, 2 * FF), C ** -0.5, 0.5),
        "down_weight": bell_draw(key_list[15], (FF, C), FF ** -0.5, 0.375),
        "token_weight": bell_draw(key_list[16], (C, CT), C ** -0.5, 0.5),
    }


EPS = 1e-05

def layer_norm(values, along=-1):
    center = lax.optimization_barrier(jnp.mean(values, along, keepdims=True))
    spread = lax.optimization_barrier(jnp.mean(jnp.square(values - center), along, keepdims=True))
    return (values - center) * lax.rsqrt(spread + EPS)

def window_view(extended):
    reach = WK // WQ
    blocks = extended.reshape((WINDOWS + reach - 1, WQ) + extended.shape[1:])
    return jnp.concatenate([blocks[offset:offset + WINDOWS] for offset in range(reach)], axis=1)

def reference(atoms_in, cond, pair, atom_mask, atom_count, atom_to_token, ada_weight, ada_bias, zero_weight, zero_bias, qkvg_weight, query_bias, pair_weight, out_weight, swiglu_weight, down_weight, token_weight):
    head_dim = C // HEADS
    margin = (WK - WQ) // 2
    positions = jnp.arange(ATOMS, dtype=jnp.int32)
    usable = (atom_mask == 1) & (positions < atom_count[0])
    cond_norm = layer_norm(cond.astype(jnp.float32)).astype(jnp.bfloat16)
    adapt = [jnp.dot(cond_norm, ada_weight[which], preferred_element_type=jnp.float32) for which in range(2)]
    gating = [jax.nn.sigmoid(jnp.dot(cond_norm, zero_weight[which], preferred_element_type=jnp.float32) + zero_bias[which]) for which in range(2)]

    def adaptive(stream, which):
        return layer_norm(stream) * jax.nn.sigmoid(adapt[which][:, :C] + ada_bias[which]) + adapt[which][:, C:]
    key_live = window_view(jnp.pad(usable, (margin, margin)))
    pair_norm = layer_norm(pair.astype(jnp.float32), 2)
    pair_bias = jnp.einsum('wicj,hc->whij', pair_norm, pair_weight, precision=lax.Precision.HIGHEST)
    factor = head_dim ** (-0.5)

    def one_sample(stream):
        attn_in = adaptive(stream.astype(jnp.float32), 0).astype(jnp.bfloat16)
        projected = jnp.dot(attn_in, qkvg_weight, preferred_element_type=jnp.float32)
        queries = ((projected[:, :C] + query_bias) * factor).astype(jnp.bfloat16)
        keyval = projected[:, C:3 * C].astype(jnp.bfloat16)
        gate_attn = jax.nn.sigmoid(projected[:, 3 * C:])
        windowed = window_view(jnp.pad(keyval, ((margin, margin), (0, 0))))
        query_win = queries.reshape(WINDOWS, WQ, HEADS, head_dim).astype(jnp.float32)
        keys_win = windowed[..., :C].reshape(WINDOWS, WK, HEADS, head_dim).astype(jnp.float32)
        values_win = windowed[..., C:].reshape(WINDOWS, WK, HEADS, head_dim).astype(jnp.float32)
        scores = jnp.einsum('wihd,wjhd->whij', query_win, keys_win) + pair_bias
        scores = jnp.where(key_live[:, None, None, :], scores, -1000000000.0)
        attention = jax.nn.softmax(scores, axis=-1).astype(jnp.bfloat16)
        weighted = jnp.einsum('whij,wjhd->wihd', attention.astype(jnp.float32), values_win).reshape(ATOMS, C)
        blended = (weighted * gate_attn).astype(jnp.bfloat16)
        after_attn = (stream.astype(jnp.float32) + gating[0] * jnp.dot(blended, out_weight, preferred_element_type=jnp.float32)).astype(jnp.bfloat16)
        trans_in = adaptive(after_attn.astype(jnp.float32), 1).astype(jnp.bfloat16)
        mixed = jnp.dot(trans_in, swiglu_weight, preferred_element_type=jnp.float32)
        hidden = (jax.nn.silu(mixed[:, :FF]) * mixed[:, FF:]).astype(jnp.bfloat16)
        result = (after_attn.astype(jnp.float32) + gating[1] * jnp.dot(hidden, down_weight, preferred_element_type=jnp.float32)).astype(jnp.bfloat16)
        features = jax.nn.relu(jnp.dot(result, token_weight, preferred_element_type=jnp.float32)).astype(jnp.bfloat16)
        masked = jnp.where(usable[:, None], features.astype(jnp.float32), jnp.zeros((), jnp.float32))
        totals = jax.ops.segment_sum(masked, atom_to_token, num_segments=TOKENS)
        return (result, totals)
    atoms_out, totals = lax.map(one_sample, atoms_in)
    counts = jax.ops.segment_sum(usable.astype(jnp.float32), atom_to_token, num_segments=TOKENS)
    tokens_out = (totals / jnp.maximum(counts, 1.0)[None, :, None]).astype(jnp.bfloat16)
    return (atoms_out, tokens_out)
```

```python
import functools

import jax
import jax.numpy as jnp
from jax import lax
from jax.experimental import pallas as pl
from jax.experimental.pallas import tpu as pltpu
from jax.sharding import PartitionSpec as P

ATOMS_PER_TOKEN = 8
EPS = 1e-05
DEAD = -1000000000.0
MESH = pl.DeviceIdType.MESH
F32 = jnp.float32
BF16 = jnp.bfloat16


def iota(shape, axis):
    return lax.broadcasted_iota(jnp.int32, shape, axis)


def mm(a, b):
    return jnp.dot(a, b, preferred_element_type=F32)


def two_pieces(values):
    high = values.astype(BF16)
    low = (values - high.astype(F32)).astype(BF16)
    return high, low


def block_body(
    n,
    atoms_ref, cond_ref, pair_ref, mask_ref, token_ref, count_ref,
    ada_ref, ada_bias_ref, zero_ref, zero_bias_ref, qkvg_ref, query_bias_ref,
    pair_weight_ref, out_ref, swiglu_ref, down_ref, token_weight_ref,
    atoms_out_ref, tokens_out_ref,
    pair_buf, halo_x, halo_c, halo_m, halo_t, kv_ref, q_ref, gate_ref, bias_ref,
    live_ref, mod_ref, feat_ref, center_ref, mean_ref, lhs_ref, fold_ref,
    edge_out, edge_in, onehot_ref, counts_ref,
    pair_sem, send_sem, recv_sem, edge_send_sem, edge_recv_sem,
):
    samples, atoms, width = atoms_ref.shape
    windows, rows_pair, key_len = pair_ref.shape
    heads, channels = pair_weight_ref.shape
    head_dim = width // heads
    query_len = rows_pair // channels
    half = query_len // 2
    margin = (key_len - query_len) // 2
    tokens = tokens_out_ref.shape[1]
    hidden = down_ref.shape[0]
    token_width = token_weight_ref.shape[1]
    rows_half = half * channels

    me = lax.axis_index("atom")
    right, left = lax.rem(me + 1, n), lax.rem(me + n - 1, n)

    groups = pair_sem.shape[0]
    per_group = windows // groups
    pair_copies = []
    for g in range(groups):
        part = pl.ds(g * per_group, per_group)
        copy = pltpu.make_async_copy(pair_ref.at[part], pair_buf.at[part], pair_sem.at[g])
        copy.start()
        pair_copies.append(copy)

    barrier = pltpu.get_barrier_semaphore()
    for neighbour in (left, right):
        pl.semaphore_signal(barrier, inc=1, device_id={"atom": neighbour}, device_id_type=MESH)
    pl.semaphore_wait(barrier, 2)

    copies = []
    for side, (target, start) in enumerate(((right, atoms - margin), (left, 0))):
        own = pl.ds(start, margin)
        for which, (src, dst) in enumerate(
            (
                (atoms_ref.at[:, own], halo_x.at[side]),
                (cond_ref.at[own], halo_c.at[side]),
                (mask_ref, halo_m.at[side]),
                (token_ref, halo_t.at[side]),
            )
        ):
            copy = pltpu.make_async_remote_copy(
                src_ref=src,
                dst_ref=dst,
                send_sem=send_sem.at[side, which],
                recv_sem=recv_sem.at[side, which],
                device_id={"atom": target},
                device_id_type=MESH,
            )
            copy.start()
            copies.append(copy)

    row, col = iota((width, width), 0), iota((width, width), 1)
    inverse = 1.0 / width
    center_ref[...] = (jnp.where(row == col, 1.0, 0.0) - inverse).astype(BF16)
    mean_ref[...] = jnp.full(mean_ref.shape, inverse, F32).astype(BF16)

    def norm(values):
        centred = mm(values, center_ref[...])
        high, low = two_pieces(centred * centred)
        spread = mm(jnp.concatenate([high, low], axis=1), mean_ref[...])
        return centred * lax.rsqrt(spread + EPS)

    cond_norm = norm(cond_ref[...]).astype(BF16)
    for which in range(2):
        adapt = mm(cond_norm, ada_ref[which])
        mod_ref[3 * which] = jax.nn.sigmoid(
            adapt[:, :width] + ada_bias_ref[which : which + 1]
        )
        mod_ref[3 * which + 1] = adapt[:, width:]
        mod_ref[3 * which + 2] = jax.nn.sigmoid(
            mm(cond_norm, zero_ref[which]) + zero_bias_ref[which : which + 1]
        )

    factor = head_dim**-0.5
    kv_ref[:, :, 2 * width :] = jnp.ones((samples, atoms + 2 * margin, width), BF16)
    for s in range(samples):
        attn_in = (norm(atoms_ref[s]) * mod_ref[0] + mod_ref[1]).astype(BF16)
        projected = mm(attn_in, qkvg_ref[...])
        q_ref[s] = ((projected[:, :width] + query_bias_ref[...]) * factor).astype(BF16)
        kv_ref[s, pl.ds(margin, atoms), pl.ds(0, 2 * width)] = projected[
            :, width : 3 * width
        ].astype(BF16)
        gate_ref[s] = jax.nn.sigmoid(projected[:, 3 * width :])

    weight = pair_weight_ref[...]
    weight = weight - jnp.mean(weight, axis=1, keepdims=True)
    row, col = iota((rows_half, rows_half), 0), iota((rows_half, rows_half), 1)
    same = jnp.where(row // channels == col // channels, 1.0 / channels, 0.0)
    lhs_ref[pl.ds(0, rows_half)] = (jnp.where(row == col, 1.0, 0.0) - same).astype(BF16)
    spread_c = jnp.where(
        iota((channels, rows_half), 1) % channels == iota((channels, rows_half), 0), 1.0, 0.0
    ).astype(BF16)
    own_query = iota((half, rows_half), 1) // channels == iota((half, rows_half), 0)
    remaining = weight
    lines = heads * half
    for piece in range(3):
        part = remaining.astype(BF16)
        remaining = remaining - part.astype(F32)
        wide = mm(part, spread_c)
        blocks = [
            jnp.where(own_query, jnp.broadcast_to(wide[h : h + 1], (half, rows_half)), 0.0)
            for h in range(heads)
        ]
        lhs_ref[pl.ds(rows_half + piece * lines, lines)] = jnp.concatenate(
            blocks, axis=0
        ).astype(BF16)
    folded = rows_half // 2
    fold_ref[...] = jnp.where(
        (iota((half, 2 * folded), 1) % folded) // (channels // 2) == iota((half, 2 * folded), 0),
        1.0 / channels,
        0.0,
    ).astype(BF16)

    def pair_window(w):
        block = pair_buf[w]
        both = jnp.concatenate([block[:rows_half], block[rows_half:]], axis=1)
        result = mm(lhs_ref[...], both)
        centred = result[:rows_half]
        at = rows_half
        total = (
            result[at : at + lines]
            + result[at + lines : at + 2 * lines]
            + result[at + 2 * lines : at + 3 * lines]
        )
        square = (centred * centred).reshape(half, 2, channels // 2, 2 * key_len)
        square = (square[:, 0] + square[:, 1]).reshape(folded, 2 * key_len)
        high, low = two_pieces(square)
        spread = mm(fold_ref[...], jnp.concatenate([high, low], axis=0))
        scale = lax.rsqrt(spread + EPS)
        bias = total * jnp.concatenate([scale] * heads, axis=0)
        bias_ref[w, pl.ds(0, lines)] = bias[:, :key_len]
        bias_ref[w, pl.ds(lines, lines)] = bias[:, key_len:]

    for g in range(groups):
        pair_copies[g].wait()

        def pair_step(i, carry, g=g):
            pair_window(g * per_group + 2 * i)
            pair_window(g * per_group + 2 * i + 1)
            return carry

        lax.fori_loop(0, per_group // 2, pair_step, 0)

    for copy in copies:
        copy.wait()
    lanes = 128
    mask_ext = jnp.concatenate(
        [halo_m[0][:, atoms - lanes :], mask_ref[...], halo_m[1][:, :lanes]], axis=1
    )
    token_ext = jnp.concatenate(
        [halo_t[0][:, atoms - lanes :], token_ref[...], halo_t[1][:, :lanes]], axis=1
    )
    extent = atoms + 2 * lanes
    position = me * atoms - lanes + iota((1, extent), 1)
    usable = (
        (mask_ext == 1)
        & (position >= 0)
        & (position < n * atoms)
        & (position < count_ref[0])
    )
    live = jnp.broadcast_to(jnp.where(usable, 1.0, 0.0), (8, extent))
    for w in range(windows):
        shift = (extent - (lanes - margin + query_len * w)) % extent
        live_ref[w] = pltpu.roll(live, shift, axis=1)[:, :key_len]
    relative = jnp.where(usable, token_ext - me * tokens, -2)
    hits = iota((tokens, extent), 0) == jnp.broadcast_to(relative, (tokens, extent))
    hits = jnp.where(hits, 1.0, 0.0)
    counts_ref[...] = jnp.broadcast_to(
        1.0 / jnp.maximum(jnp.sum(hits, axis=1, keepdims=True), 1.0), counts_ref.shape
    )
    onehot_ref[...] = hits[:, lanes : lanes + atoms].astype(BF16)
    relative8 = jnp.broadcast_to(relative[:, lanes : lanes + atoms], (8, atoms))
    rolled8 = pltpu.roll(relative8, query_len, axis=1)
    lower_hit = jnp.where(relative8[:, :lanes] == -1, 1.0, 0.0).astype(BF16)[:, :query_len]
    upper_hit = jnp.where(rolled8[:, :lanes] == tokens, 1.0, 0.0).astype(BF16)[:, :query_len]

    for side in range(2):
        inside = (me > 0) if side == 0 else (me < n - 1)
        cond_halo = norm(halo_c[side]).astype(BF16)
        adapt = mm(cond_halo, ada_ref[0])
        scale = jax.nn.sigmoid(adapt[:, :width] + ada_bias_ref[0:1])
        shift = adapt[:, width:]
        normed = norm(halo_x[side].reshape(samples * margin, width))
        attn_in = (normed.reshape(samples, margin, width) * scale[None] + shift[None]).astype(BF16)
        projected = mm(
            attn_in.reshape(samples * margin, width), qkvg_ref[:, pl.ds(width, 2 * width)]
        )
        projected = jnp.where(inside, projected, 0.0).astype(BF16)
        start = 0 if side == 0 else margin + atoms
        kv_ref[:, pl.ds(start, margin), pl.ds(0, 2 * width)] = projected.reshape(
            samples, margin, 2 * width
        )

    head_of = iota((half, width), 1) // head_dim

    def attend(s, w):
        rows = pl.ds(pl.multiple_of(w * query_len, query_len), query_len)
        keys = pl.ds(pl.multiple_of(w * query_len, query_len), key_len)
        query = q_ref[s, rows]
        parts = []
        for side in range(2):
            piece = query[side * half : (side + 1) * half]
            for h in range(heads):
                parts.append(jnp.where(head_of == h, piece, jnp.zeros_like(piece)))
        stacked = jnp.concatenate(parts, axis=0)
        scores = lax.dot_general(
            stacked,
            kv_ref[s, keys, pl.ds(0, width)],
            (((1,), (1,)), ((), ())),
            preferred_element_type=F32,
        )
        scores = jnp.where(live_ref[w][0:1] > 0.5, scores + bias_ref[w], DEAD)
        top = jnp.max(scores, axis=1, keepdims=True)
        weights = jnp.exp(scores - top).astype(BF16)
        mixed = mm(weights, kv_ref[s, keys, pl.ds(width, 2 * width)])
        outs = []
        for side in range(2):
            base = side * heads * half
            value = mixed[base : base + half, :width]
            amount = mixed[base : base + half, width:]
            for h in range(1, heads):
                at = base + h * half
                value = jnp.where(head_of == h, mixed[at : at + half, :width], value)
                amount = jnp.where(head_of == h, mixed[at : at + half, width:], amount)
            outs.append(value / amount)
        return (jnp.concatenate(outs, axis=0) * gate_ref[s, rows]).astype(BF16)

    def process(pairs):
        rows = [pl.ds(pl.multiple_of(w * query_len, query_len), query_len) for w in pairs]
        order = [(s, i) for s in range(samples) for i in range(len(pairs))]

        def modulation(k):
            one = jnp.concatenate([mod_ref[k, r] for r in rows], axis=0)
            return jnp.concatenate([one] * samples, axis=0)

        blended = jnp.concatenate([attend(s, pairs[i]) for s, i in order], axis=0)
        stream = jnp.concatenate([atoms_ref[s, rows[i]] for s, i in order], axis=0).astype(F32)
        after = (stream + modulation(2) * mm(blended, out_ref[...])).astype(BF16)
        trans_in = (norm(after) * modulation(3) + modulation(4)).astype(BF16)
        mixed = mm(trans_in, swiglu_ref[...])
        units = (jax.nn.silu(mixed[:, :hidden]) * mixed[:, hidden:]).astype(BF16)
        final = (after.astype(F32) + modulation(5) * mm(units, down_ref[...])).astype(BF16)
        features = jnp.maximum(mm(final, token_weight_ref[...]), 0.0).astype(BF16)
        for place, (s, i) in enumerate(order):
            at = place * query_len
            atoms_out_ref[s, rows[i]] = final[at : at + query_len]
            feat_ref[s, rows[i]] = features[at : at + query_len]
        return features

    features = process([0, windows - 1])
    sample_row = iota((8, token_width), 0)
    for side, hit in enumerate((upper_hit, lower_hit)):
        place = 1 - side
        total = jnp.zeros((8, token_width), F32)
        for s in range(samples):
            at = (2 * s + place) * query_len
            total = jnp.where(sample_row == s, mm(hit, features[at : at + query_len]), total)
        edge_out[side] = total
    edge_copies = []
    for side, target in enumerate((right, left)):
        copy = pltpu.make_async_remote_copy(
            src_ref=edge_out.at[side],
            dst_ref=edge_in.at[side],
            send_sem=edge_send_sem.at[side],
            recv_sem=edge_recv_sem.at[side],
            device_id={"atom": target},
            device_id_type=MESH,
        )
        copy.start()
        edge_copies.append(copy)

    def middle(i, carry):
        process([2 * i + 1, 2 * i + 2])
        return carry

    lax.fori_loop(0, (windows - 2) // 2, middle, 0)

    for copy in edge_copies:
        copy.wait()
    token_row = iota((tokens, token_width), 0)
    per_count = counts_ref[:, 0:1]
    for s in range(samples):
        total = mm(onehot_ref[...], feat_ref[s])
        from_left = jnp.where(me > 0, edge_in[0, s : s + 1], 0.0)
        from_right = jnp.where(me < n - 1, edge_in[1, s : s + 1], 0.0)
        total = total + jnp.where(token_row == 0, from_left, 0.0)
        total = total + jnp.where(token_row == tokens - 1, from_right, 0.0)
        tokens_out_ref[s] = (total * per_count).astype(BF16)


def on_device(
    n,
    atoms_in, cond, pair, atom_mask, atom_count, atom_to_token, ada_weight, ada_bias,
    zero_weight, zero_bias, qkvg_weight, query_bias, pair_weight, out_weight,
    swiglu_weight, down_weight, token_weight,
):
    samples, atoms, width = atoms_in.shape
    windows, query_len, channels, key_len = pair.shape
    heads = pair_weight.shape[0]
    margin = (key_len - query_len) // 2
    tokens = atoms // ATOMS_PER_TOKEN
    token_width = token_weight.shape[1]
    half = query_len // 2
    rows_half = half * channels
    groups = 3 if windows % 6 == 0 else 1
    vmem = pl.BlockSpec(memory_space=pltpu.VMEM)
    smem = pl.BlockSpec(memory_space=pltpu.SMEM)
    return pl.pallas_call(
        functools.partial(block_body, n),
        out_shape=(
            jax.ShapeDtypeStruct(atoms_in.shape, BF16),
            jax.ShapeDtypeStruct((samples, tokens, token_width), BF16),
        ),
        in_specs=[vmem, vmem, pl.BlockSpec(memory_space=pl.ANY), vmem, vmem, smem] + [vmem] * 11,
        out_specs=(vmem, vmem),
        scratch_shapes=[
            pltpu.VMEM((windows, query_len * channels, key_len), BF16),
            pltpu.VMEM((2, samples, margin, width), BF16),
            pltpu.VMEM((2, margin, width), BF16),
            pltpu.VMEM((2, 1, atoms), jnp.int32),
            pltpu.VMEM((2, 1, atoms), jnp.int32),
            pltpu.VMEM((samples, atoms + 2 * margin, 3 * width), BF16),
            pltpu.VMEM((samples, atoms, width), BF16),
            pltpu.VMEM((samples, atoms, width), F32),
            pltpu.VMEM((windows, heads * query_len, key_len), F32),
            pltpu.VMEM((windows, 8, key_len), F32),
            pltpu.VMEM((6, atoms, width), F32),
            pltpu.VMEM((samples, atoms, token_width), BF16),
            pltpu.VMEM((width, width), BF16),
            pltpu.VMEM((2 * width, width), BF16),
            pltpu.VMEM((rows_half + 3 * heads * half, rows_half), BF16),
            pltpu.VMEM((half, rows_half), BF16),
            pltpu.VMEM((2, 8, token_width), F32),
            pltpu.VMEM((2, 8, token_width), F32),
            pltpu.VMEM((tokens, atoms), BF16),
            pltpu.VMEM((tokens, 128), F32),
            pltpu.SemaphoreType.DMA((groups,)),
            pltpu.SemaphoreType.DMA((2, 4)),
            pltpu.SemaphoreType.DMA((2, 4)),
            pltpu.SemaphoreType.DMA((2,)),
            pltpu.SemaphoreType.DMA((2,)),
        ],
        compiler_params=pltpu.CompilerParams(collective_id=0, has_side_effects=True),
        name="atom_block",
    )(
        atoms_in, cond, pair.reshape(windows, query_len * channels, key_len),
        atom_mask.reshape(1, atoms), atom_to_token.reshape(1, atoms), atom_count,
        ada_weight, ada_bias, zero_weight, zero_bias, qkvg_weight,
        query_bias.reshape(1, width), pair_weight, out_weight, swiglu_weight,
        down_weight, token_weight,
    )


def solution(mesh):
    shard = P(("struct", "atom"))
    stream = P("struct", "atom", None)
    in_specs = (stream, shard, shard, shard, P("struct"), shard) + (P(),) * 11
    return jax.shard_map(
        functools.partial(on_device, mesh.shape["atom"]),
        mesh=mesh,
        in_specs=in_specs,
        out_specs=(stream, stream),
        check_vma=False,
    )
```

```python
import functools

import jax
import jax.numpy as jnp
from jax import lax
from jax.experimental import pallas as pl
from jax.experimental.pallas import tpu as pltpu
from jax.sharding import PartitionSpec as P

ATOMS_PER_TOKEN = 8
EPS = 1e-05
STEPS = 1
DEAD = -1000000000.0
MESH = pl.DeviceIdType.MESH
F32 = jnp.float32
BF16 = jnp.bfloat16


def iota(shape, axis):
    return lax.broadcasted_iota(jnp.int32, shape, axis)


def mm(a, b):
    return jnp.dot(a, b, preferred_element_type=F32)


def two_pieces(values):
    high = values.astype(BF16)
    low = (values - high.astype(F32)).astype(BF16)
    return high, low


def block_body(
    n,
    atoms_hbm, cond_hbm, pair_ref, mask_ref, token_ref, count_ref,
    ada_hbm, ada_bias_hbm, zero_hbm, zero_bias_hbm, qkvg_hbm, query_bias_hbm,
    pair_weight_hbm, out_hbm, swiglu_hbm, down_hbm, token_weight_hbm,
    atoms_out_ref, tokens_out_ref,
    atoms_ref, cond_ref, ada_ref, ada_bias_ref, zero_ref, zero_bias_ref, qkvg_ref,
    query_bias_ref, pair_weight_ref, out_ref, swiglu_ref, down_ref, token_weight_ref,
    pair_buf, halo_x, halo_c, halo_m0, halo_m1, halo_t0, halo_t1, kv_ref, q_ref, gate_ref, bias_ref,
    live_ref, mod_ref, feat_ref, center_ref, mean_ref, lhs_ref, fold_ref,
    edge_out, edge_in, onehot_ref, counts_ref,
    load_sem, pair_sem, send_sem, recv_sem, edge_send_sem, edge_recv_sem,
):
    samples, atoms, width = atoms_ref.shape
    windows, rows_pair, key_len = pair_ref.shape
    heads, channels = pair_weight_ref.shape
    head_dim = width // heads
    query_len = rows_pair // channels
    half = query_len // 2
    margin = (key_len - query_len) // 2
    tokens = tokens_out_ref.shape[1]
    hidden = down_ref.shape[0]
    token_width = token_weight_ref.shape[1]
    rows_half = half * channels

    halo_m, halo_t = (halo_m0, halo_m1), (halo_t0, halo_t1)
    me = lax.axis_index("atom")
    right, left = lax.rem(me + 1, n), lax.rem(me + n - 1, n)

    early = (
        (cond_hbm, cond_ref), (atoms_hbm, atoms_ref), (ada_hbm, ada_ref),
        (ada_bias_hbm, ada_bias_ref), (zero_hbm, zero_ref), (zero_bias_hbm, zero_bias_ref),
        (qkvg_hbm, qkvg_ref), (query_bias_hbm, query_bias_ref),
        (pair_weight_hbm, pair_weight_ref),
    )
    late = (
        (out_hbm, out_ref), (swiglu_hbm, swiglu_ref), (down_hbm, down_ref),
        (token_weight_hbm, token_weight_ref),
    )
    loads = [
        pltpu.make_async_copy(src, dst, load_sem.at[i])
        for i, (src, dst) in enumerate(early + late)
    ]
    for copy in loads[: len(early)]:
        copy.start()
    groups = pair_sem.shape[0]
    per_group = windows // groups
    pair_copies = []
    for g in range(groups):
        part = pl.ds(g * per_group, per_group)
        copy = pltpu.make_async_copy(pair_ref.at[part], pair_buf.at[part], pair_sem.at[g])
        copy.start()
        pair_copies.append(copy)
    for copy in loads[len(early) :]:
        copy.start()

    barrier = pltpu.get_barrier_semaphore()
    for neighbour in (left, right):
        pl.semaphore_signal(barrier, inc=1, device_id={"atom": neighbour}, device_id_type=MESH)
    pl.semaphore_wait(barrier, 2)

    copies = []
    for side, (target, start) in enumerate(((right, atoms - margin), (left, 0))):
        own = pl.ds(start, margin)
        for which, (src, dst) in enumerate(
            (
                (atoms_hbm.at[:, own], halo_x.at[side]),
                (cond_hbm.at[own], halo_c.at[side]),
                (mask_ref, halo_m[side]),
                (token_ref, halo_t[side]),
            )
        ):
            copy = pltpu.make_async_remote_copy(
                src_ref=src,
                dst_ref=dst,
                send_sem=send_sem.at[side, which],
                recv_sem=recv_sem.at[side, which],
                device_id={"atom": target},
                device_id_type=MESH,
            )
            copy.start()
            copies.append(copy)

    row, col = iota((width, width), 0), iota((width, width), 1)
    inverse = 1.0 / width
    center_ref[...] = (jnp.where(row == col, 1.0, 0.0) - inverse).astype(BF16)
    mean_ref[...] = jnp.full(mean_ref.shape, inverse, F32).astype(BF16)

    for copy in loads[: len(early)]:
        copy.wait()

    def norm(values):
        centred = mm(values, center_ref[...])
        high, low = two_pieces(centred * centred)
        spread = mm(jnp.concatenate([high, low], axis=1), mean_ref[...])
        return centred * lax.rsqrt(spread + EPS)

    cond_norm = norm(cond_ref[...]).astype(BF16)
    for which in range(2):
        adapt = mm(cond_norm, ada_ref[which])
        mod_ref[3 * which] = jax.nn.sigmoid(
            adapt[:, :width] + ada_bias_ref[which : which + 1]
        )
        mod_ref[3 * which + 1] = adapt[:, width:]
        mod_ref[3 * which + 2] = jax.nn.sigmoid(
            mm(cond_norm, zero_ref[which]) + zero_bias_ref[which : which + 1]
        )

    factor = head_dim**-0.5
    kv_ref[:, :, 2 * width :] = jnp.ones((samples, atoms + 2 * margin, width), BF16)
    for s in range(samples):
        attn_in = (norm(atoms_ref[s]) * mod_ref[0] + mod_ref[1]).astype(BF16)
        projected = mm(attn_in, qkvg_ref[...])
        q_ref[s] = ((projected[:, :width] + query_bias_ref[...]) * factor).astype(BF16)
        kv_ref[s, pl.ds(margin, atoms), pl.ds(0, 2 * width)] = projected[
            :, width : 3 * width
        ].astype(BF16)
        gate_ref[s] = jax.nn.sigmoid(projected[:, 3 * width :])

    weight = pair_weight_ref[...]
    weight = weight - jnp.mean(weight, axis=1, keepdims=True)
    row, col = iota((rows_half, rows_half), 0), iota((rows_half, rows_half), 1)
    same = jnp.where(row // channels == col // channels, 1.0 / channels, 0.0)
    lhs_ref[pl.ds(0, rows_half)] = (jnp.where(row == col, 1.0, 0.0) - same).astype(BF16)
    spread_c = jnp.where(
        iota((channels, rows_half), 1) % channels == iota((channels, rows_half), 0), 1.0, 0.0
    ).astype(BF16)
    own_query = iota((half, rows_half), 1) // channels == iota((half, rows_half), 0)
    remaining = weight
    lines = heads * half
    for piece in range(3):
        part = remaining.astype(BF16)
        remaining = remaining - part.astype(F32)
        wide = mm(part, spread_c)
        blocks = [
            jnp.where(own_query, jnp.broadcast_to(wide[h : h + 1], (half, rows_half)), 0.0)
            for h in range(heads)
        ]
        lhs_ref[pl.ds(rows_half + piece * lines, lines)] = jnp.concatenate(
            blocks, axis=0
        ).astype(BF16)
    folded = rows_half // 2
    fold_ref[...] = jnp.where(
        (iota((half, 2 * folded), 1) % folded) // (channels // 2) == iota((half, 2 * folded), 0),
        1.0 / channels,
        0.0,
    ).astype(BF16)

    def pair_window(w):
        block = pair_buf[w]
        both = jnp.concatenate([block[:rows_half], block[rows_half:]], axis=1)
        result = mm(lhs_ref[...], both)
        centred = result[:rows_half]
        at = rows_half
        total = (
            result[at : at + lines]
            + result[at + lines : at + 2 * lines]
            + result[at + 2 * lines : at + 3 * lines]
        )
        square = (centred * centred).reshape(half, 2, channels // 2, 2 * key_len)
        square = (square[:, 0] + square[:, 1]).reshape(folded, 2 * key_len)
        high, low = two_pieces(square)
        spread = mm(fold_ref[...], jnp.concatenate([high, low], axis=0))
        scale = lax.rsqrt(spread + EPS)
        bias = total * jnp.concatenate([scale] * heads, axis=0)
        bias_ref[w, pl.ds(0, lines)] = bias[:, :key_len]
        bias_ref[w, pl.ds(lines, lines)] = bias[:, key_len:]

    for g in range(groups):
        pair_copies[g].wait()

        def pair_step(i, carry, g=g):
            pair_window(g * per_group + 2 * i)
            pair_window(g * per_group + 2 * i + 1)
            return carry

        lax.fori_loop(0, per_group // 2, pair_step, 0)

    for copy in copies:
        copy.wait()
    lanes = 128

    def as_row(ref):
        return ref[...].reshape(1, atoms)

    mask_ext = jnp.concatenate(
        [as_row(halo_m[0])[:, atoms - lanes :], as_row(mask_ref), as_row(halo_m[1])[:, :lanes]],
        axis=1,
    )
    token_ext = jnp.concatenate(
        [as_row(halo_t[0])[:, atoms - lanes :], as_row(token_ref), as_row(halo_t[1])[:, :lanes]],
        axis=1,
    )
    extent = atoms + 2 * lanes
    position = me * atoms - lanes + iota((1, extent), 1)
    usable = (
        (mask_ext == 1)
        & (position >= 0)
        & (position < n * atoms)
        & (position < count_ref[0])
    )
    live = jnp.broadcast_to(jnp.where(usable, 1.0, 0.0), (8, extent))
    for w in range(windows):
        shift = (extent - (lanes - margin + query_len * w)) % extent
        live_ref[w] = pltpu.roll(live, shift, axis=1)[:, :key_len]
    relative = jnp.where(usable, token_ext - me * tokens, -2)
    hits = iota((tokens, extent), 0) == jnp.broadcast_to(relative, (tokens, extent))
    hits = jnp.where(hits, 1.0, 0.0)
    counts_ref[...] = jnp.broadcast_to(
        1.0 / jnp.maximum(jnp.sum(hits, axis=1, keepdims=True), 1.0), counts_ref.shape
    )
    onehot_ref[...] = hits[:, lanes : lanes + atoms].astype(BF16)
    relative8 = jnp.broadcast_to(relative[:, lanes : lanes + atoms], (8, atoms))
    rolled8 = pltpu.roll(relative8, query_len, axis=1)
    lower_hit = jnp.where(relative8[:, :lanes] == -1, 1.0, 0.0).astype(BF16)[:, :query_len]
    upper_hit = jnp.where(rolled8[:, :lanes] == tokens, 1.0, 0.0).astype(BF16)[:, :query_len]

    for side in range(2):
        inside = (me > 0) if side == 0 else (me < n - 1)
        cond_halo = norm(halo_c[side]).astype(BF16)
        adapt = mm(cond_halo, ada_ref[0])
        scale = jax.nn.sigmoid(adapt[:, :width] + ada_bias_ref[0:1])
        shift = adapt[:, width:]
        normed = norm(halo_x[side].reshape(samples * margin, width))
        attn_in = (normed.reshape(samples, margin, width) * scale[None] + shift[None]).astype(BF16)
        projected = mm(
            attn_in.reshape(samples * margin, width), qkvg_ref[:, pl.ds(width, 2 * width)]
        )
        projected = jnp.where(inside, projected, 0.0).astype(BF16)
        start = 0 if side == 0 else margin + atoms
        kv_ref[:, pl.ds(start, margin), pl.ds(0, 2 * width)] = projected.reshape(
            samples, margin, 2 * width
        )

    head_of = iota((half, width), 1) // head_dim

    def attend(s, w):
        rows = pl.ds(pl.multiple_of(w * query_len, query_len), query_len)
        keys = pl.ds(pl.multiple_of(w * query_len, query_len), key_len)
        query = q_ref[s, rows]
        parts = []
        for side in range(2):
            piece = query[side * half : (side + 1) * half]
            for h in range(heads):
                parts.append(jnp.where(head_of == h, piece, jnp.zeros_like(piece)))
        stacked = jnp.concatenate(parts, axis=0)
        scores = lax.dot_general(
            stacked,
            kv_ref[s, keys, pl.ds(0, width)],
            (((1,), (1,)), ((), ())),
            preferred_element_type=F32,
        )
        scores = jnp.where(live_ref[w][0:1] > 0.5, scores + bias_ref[w], DEAD)
        top = jnp.max(scores, axis=1, keepdims=True)
        weights = jnp.exp(scores - top).astype(BF16)
        mixed = mm(weights, kv_ref[s, keys, pl.ds(width, 2 * width)])
        outs = []
        for side in range(2):
            base = side * heads * half
            value = mixed[base : base + half, :width]
            amount = mixed[base : base + half, width:]
            for h in range(1, heads):
                at = base + h * half
                value = jnp.where(head_of == h, mixed[at : at + half, :width], value)
                amount = jnp.where(head_of == h, mixed[at : at + half, width:], amount)
            outs.append(value / amount)
        return (jnp.concatenate(outs, axis=0) * gate_ref[s, rows]).astype(BF16)

    def process(pairs):
        rows = [pl.ds(pl.multiple_of(w * query_len, query_len), query_len) for w in pairs]
        order = [(s, i) for s in range(samples) for i in range(len(pairs))]

        def modulation(k):
            one = jnp.concatenate([mod_ref[k, r] for r in rows], axis=0)
            return jnp.concatenate([one] * samples, axis=0)

        blended = jnp.concatenate([attend(s, pairs[i]) for s, i in order], axis=0)
        stream = jnp.concatenate([atoms_ref[s, rows[i]] for s, i in order], axis=0).astype(F32)
        after = (stream + modulation(2) * mm(blended, out_ref[...])).astype(BF16)
        trans_in = (norm(after) * modulation(3) + modulation(4)).astype(BF16)
        mixed = mm(trans_in, swiglu_ref[...])
        units = (jax.nn.silu(mixed[:, :hidden]) * mixed[:, hidden:]).astype(BF16)
        final = (after.astype(F32) + modulation(5) * mm(units, down_ref[...])).astype(BF16)
        features = jnp.maximum(mm(final, token_weight_ref[...]), 0.0).astype(BF16)
        for place, (s, i) in enumerate(order):
            at = place * query_len
            atoms_out_ref[s, rows[i]] = final[at : at + query_len]
            feat_ref[s, rows[i]] = features[at : at + query_len]
        return features

    for copy in loads[len(early) :]:
        copy.wait()

    features = process([0, windows - 1])
    sample_row = iota((8, token_width), 0)
    for side, hit in enumerate((upper_hit, lower_hit)):
        place = 1 - side
        total = jnp.zeros((8, token_width), F32)
        for s in range(samples):
            at = (2 * s + place) * query_len
            total = jnp.where(sample_row == s, mm(hit, features[at : at + query_len]), total)
        edge_out[side] = total
    edge_copies = []
    for side, target in enumerate((right, left)):
        copy = pltpu.make_async_remote_copy(
            src_ref=edge_out.at[side],
            dst_ref=edge_in.at[side],
            send_sem=edge_send_sem.at[side],
            recv_sem=edge_recv_sem.at[side],
            device_id={"atom": target},
            device_id_type=MESH,
        )
        copy.start()
        edge_copies.append(copy)

    def middle(i, carry):
        process([per_step * i + 1 + j for j in range(per_step)])
        return carry

    per_step = (windows - 2) // STEPS
    lax.fori_loop(0, STEPS, middle, 0)

    for copy in edge_copies:
        copy.wait()
    token_row = iota((tokens, token_width), 0)
    per_count = counts_ref[:, 0:1]
    for s in range(samples):
        total = mm(onehot_ref[...], feat_ref[s])
        from_left = jnp.where(me > 0, edge_in[0, s : s + 1], 0.0)
        from_right = jnp.where(me < n - 1, edge_in[1, s : s + 1], 0.0)
        total = total + jnp.where(token_row == 0, from_left, 0.0)
        total = total + jnp.where(token_row == tokens - 1, from_right, 0.0)
        tokens_out_ref[s] = (total * per_count).astype(BF16)


def on_device(
    n,
    atoms_in, cond, pair, atom_mask, atom_count, atom_to_token, ada_weight, ada_bias,
    zero_weight, zero_bias, qkvg_weight, query_bias, pair_weight, out_weight,
    swiglu_weight, down_weight, token_weight,
):
    samples, atoms, width = atoms_in.shape
    windows, query_len, channels, key_len = pair.shape
    heads = pair_weight.shape[0]
    margin = (key_len - query_len) // 2
    tokens = atoms // ATOMS_PER_TOKEN
    token_width = token_weight.shape[1]
    half = query_len // 2
    rows_half = half * channels
    groups = 3 if windows % 6 == 0 else 1
    vmem = pl.BlockSpec(memory_space=pltpu.VMEM)
    hbm = pl.BlockSpec(memory_space=pltpu.HBM)
    query_bias = query_bias.reshape(1, width)
    staged = (
        atoms_in, cond, ada_weight, ada_bias, zero_weight, zero_bias, qkvg_weight,
        query_bias, pair_weight, out_weight, swiglu_weight, down_weight, token_weight,
    )
    smem = pl.BlockSpec(memory_space=pltpu.SMEM)
    return pl.pallas_call(
        functools.partial(block_body, n),
        out_shape=(
            pltpu.VMEM(atoms_in.shape, BF16),
            pltpu.VMEM((samples, tokens, token_width), BF16),
        ),
        in_specs=[hbm, hbm, hbm, vmem, vmem, smem] + [hbm] * 11,
        out_specs=(vmem, vmem),
        scratch_shapes=[pltpu.VMEM(a.shape, a.dtype) for a in staged]
        + [
            pltpu.VMEM((windows, query_len * channels, key_len), BF16),
            pltpu.VMEM((2, samples, margin, width), BF16),
            pltpu.VMEM((2, margin, width), BF16),
            pltpu.VMEM((atoms,), jnp.int32),
            pltpu.VMEM((atoms,), jnp.int32),
            pltpu.VMEM((atoms,), jnp.int32),
            pltpu.VMEM((atoms,), jnp.int32),
            pltpu.VMEM((samples, atoms + 2 * margin, 3 * width), BF16),
            pltpu.VMEM((samples, atoms, width), BF16),
            pltpu.VMEM((samples, atoms, width), F32),
            pltpu.VMEM((windows, heads * query_len, key_len), F32),
            pltpu.VMEM((windows, 8, key_len), F32),
            pltpu.VMEM((6, atoms, width), F32),
            pltpu.VMEM((samples, atoms, token_width), BF16),
            pltpu.VMEM((width, width), BF16),
            pltpu.VMEM((2 * width, width), BF16),
            pltpu.VMEM((rows_half + 3 * heads * half, rows_half), BF16),
            pltpu.VMEM((half, rows_half), BF16),
            pltpu.VMEM((2, 8, token_width), F32),
            pltpu.VMEM((2, 8, token_width), F32),
            pltpu.VMEM((tokens, atoms), BF16),
            pltpu.VMEM((tokens, 128), F32),
            pltpu.SemaphoreType.DMA((len(staged),)),
            pltpu.SemaphoreType.DMA((groups,)),
            pltpu.SemaphoreType.DMA((2, 4)),
            pltpu.SemaphoreType.DMA((2, 4)),
            pltpu.SemaphoreType.DMA((2,)),
            pltpu.SemaphoreType.DMA((2,)),
        ],
        compiler_params=pltpu.CompilerParams(collective_id=0, has_side_effects=True),
        name="atom_block",
    )(
        atoms_in, cond, pair.reshape(windows, query_len * channels, key_len),
        atom_mask, atom_to_token, atom_count,
        ada_weight, ada_bias, zero_weight, zero_bias, qkvg_weight,
        query_bias, pair_weight, out_weight, swiglu_weight,
        down_weight, token_weight,
    )


def solution(mesh):
    shard = P(("struct", "atom"))
    stream = P("struct", "atom", None)
    in_specs = (stream, shard, shard, shard, P("struct"), shard) + (P(),) * 11
    return jax.shard_map(
        functools.partial(on_device, mesh.shape["atom"]),
        mesh=mesh,
        in_specs=in_specs,
        out_specs=(stream, stream),
        check_vma=False,
    )
```
